256 devices in a mesh: tile: 32 (over y, z), grp: 8 (over x, core).
Axes of the slice: x: 4, y: 4, z: 8, core: 2. Of those that a mesh axis runs over, the one named last changes fastest.
Arguments:
- basis: float32 [131072, 2401], P(('tile', 'grp')), may hold values from -6 to 6
- pixel_ids: int32 [2097152], P(('tile', 'grp')), may hold values from 0 to 511
- band_ids: int32 [2097152], P(('tile', 'grp')), may hold values from 0 to 4
- mags: float32 [2097152], P(('tile', 'grp')), may hold values from -6 to 6
- inv_var: float32 [2097152], P(('tile', 'grp')), may hold values from 0.01 to 10
Outputs:
- solution: float32 [5, 2401], replicated
- residual: float32 [5, 2401], replicated
The draws below stay inside these ranges and needn't reach their ends.
All inputs are finite; a program needn't handle non-finite values.
Results may differ from the reference program's by a relative error of at most 0.0003.
Values sent between devices are 32-bit elements; how exact they have to be, the bound alone decides.
No kernel may reach another device: no remote copies, remote signals or barrier semaphores. Data moves between devices by JAX's collectives and lax.ppermute only.
A program may use at most 64 MiB of HBM per device.

```python
import math
import jax
import jax.numpy as jnp
from jax import lax

BANDS = 5
NCOEF = 2401
PIX_DEV = 512
OBJ_DEV = 8192
ITERS = 3
PIXELS = 131072
OBJECTS = 2097152


def touch_ends(entries, rng, least, top_value):
    extent = entries.shape
    place = [jax.random.randint(jax.random.fold_in(rng, axis), (), 0, extent[axis]) for axis in range(len(extent))]
    entries = entries.at[tuple(place)].set(least)
    longest = extent.index(max(extent))
    place[longest] = (place[longest] + 1) % extent[longest]
    return entries.at[tuple(place)].set(top_value)


def block_levels(key, dims, cuts, low, largest):
    def one(position, parts):
        steps = jax.random.uniform(jax.random.fold_in(jax.random.fold_in(key, 6), position), (parts,), jnp.float32, low / len(cuts), largest / len(cuts))
        return jnp.repeat(jnp.exp(steps), dims[position] // parts).reshape((-1,) + (1,) * (len(dims) - position - 1))

    factor_of = one(*cuts[0])
    for cut in cuts[1:]:
        factor_of = factor_of * one(*cut)
    return factor_of


def centred(stream_key, dims, scale, limit, cuts=(), kind=jnp.bfloat16):
    level = block_levels(stream_key, dims, cuts, -0.22, 0.18) if cuts else 1.0
    entries = jax.random.normal(stream_key, dims, jnp.float32) * scale * level
    return jnp.minimum(jnp.maximum(entries, -limit), limit).astype(kind)


def setup_inputs(seed: int = 0) -> dict:
    key_list = jax.random.split(jax.random.key(seed), 6)
    basis = centred(key_list[0], (PIXELS, NCOEF), 1.0, 6.0, ((0, 256),), jnp.float32)
    pixel_ids = touch_ends(jax.random.randint(key_list[1], (OBJECTS,), 0, PIX_DEV), jax.random.fold_in(key_list[1], 1), 0, PIX_DEV - 1).astype(jnp.int32)
    band_ids = touch_ends(jax.random.randint(key_list[2], (OBJECTS,), 0, BANDS), jax.random.fold_in(key_list[2], 1), 0, BANDS - 1).astype(jnp.int32)
    mags = centred(key_list[3], (OBJECTS,), 1.0, 6.0, ((0, 256),), jnp.float32)
    inv_var = jnp.clip(jnp.exp(math.log(10.0) - 6.9077553 * jax.random.uniform(key_list[4], (OBJECTS,), jnp.float32) ** block_levels(key_list[4], (OBJECTS,), ((0, 256),), -0.2, 0.2)), 0.01, 10.0)
    return {"basis": basis, "pixel_ids": pixel_ids, "band_ids": band_ids, "mags": mags, "inv_var": inv_var}


ridge = 0.1

def reference(basis, pixel_ids, band_ids, mags, inv_var):
    total = basis.shape[0]
    rows = pixel_ids.shape[0]
    owner = jnp.arange(rows, dtype=jnp.int32) // OBJ_DEV * PIX_DEV
    segment = (band_ids * total + pixel_ids + owner).astype(jnp.int32)
    counts = jax.ops.segment_sum(inv_var, segment, num_segments=BANDS * total).reshape(BANDS, total)
    weighted = jax.ops.segment_sum(inv_var * mags, segment, num_segments=BANDS * total).reshape(BANDS, total)
    block = math.gcd(total, 32768)
    nblocks = total // block
    blocks = basis.reshape(nblocks, block, NCOEF)
    count_blocks = jnp.transpose(counts.reshape(BANDS, nblocks, block), (1, 0, 2))
    weight_blocks = jnp.transpose(weighted.reshape(BANDS, nblocks, block), (1, 0, 2))

    def rhs_step(acc, pieces):
        tiles, weights = pieces
        return (acc + jnp.dot(weights, tiles, precision=lax.Precision.HIGHEST), None)
    zero = jnp.zeros((BANDS, NCOEF), jnp.float32)
    local_rhs, _ = lax.scan(rhs_step, zero, (blocks, weight_blocks))
    right_side = local_rhs / jnp.sqrt(jnp.float32(total))

    def apply_op(direction):

        def op_step(acc, pieces):
            tiles, cnt = pieces
            model = jnp.dot(direction, tiles.T, precision=lax.Precision.HIGHEST)
            scaled = cnt * model
            return (acc + jnp.dot(scaled, tiles, precision=lax.Precision.HIGHEST), None)
        summed, _ = lax.scan(op_step, zero, (blocks, count_blocks))
        return summed / jnp.float32(total) + ridge * direction
    solution = zero
    residual = right_side
    direction = right_side
    norm_now = jnp.sum(residual * residual)
    for step in range(ITERS):
        image = apply_op(direction)
        step_len = norm_now / jnp.sum(direction * image)
        solution = solution + step_len * direction
        residual = residual - step_len * image
        norm_next = jnp.sum(residual * residual)
        direction = residual + norm_next / norm_now * direction
        norm_now = norm_next
    return (solution, residual)
```

```python
import functools

import jax
import jax.numpy as jnp
from jax import lax
from jax.experimental import pallas as pl
from jax.experimental.pallas import tpu as pltpu
from jax.sharding import Mesh
from jax.sharding import PartitionSpec as P

BANDS = 5
ITERS = 3
AXES = ("y", "z", "x", "c")
SPAN = {"y": 4, "z": 8, "x": 4, "c": 2}
RIDGE = 0.1
PIX = 512
NCOEF = 2401
LANES = 128
TILES = -(-NCOEF // LANES)
WIDE = TILES * LANES
ROWS = 96
HALF = ROWS // 2
OBJ_ROWS = 64
STRIPES = PIX // LANES
NT = (((1,), (1,)), ((), ()))
NN = (((1,), (0,)), ((), ()))
F32, BF16 = jnp.float32, jnp.bfloat16


def dot(a, b, dims):
    return lax.dot_general(a, b, dims, preferred_element_type=F32)


def split(x):
    high = x.astype(BF16)
    return high, (x - high.astype(F32)).astype(BF16)


def image_of(scaled, high_ref, low_ref, core_ref, full, mine_ref, other_ref):
    both = jnp.concatenate(split(scaled), axis=0)
    total = dot(high_ref[...], both, NT) + dot(low_ref[...], both, NT)
    for j in range(TILES):
        turned = total[j * LANES : (j + 1) * LANES, :].T
        full[j * BANDS : (j + 1) * BANDS, :] = turned[:BANDS] + turned[8 : 8 + BANDS]
    full[TILES * BANDS :, :] = jnp.zeros((ROWS - TILES * BANDS, LANES), F32)
    first = core_ref[0:1, :] == 0
    for out, one, two in ((mine_ref, 0, HALF), (other_ref, HALF, 0)):
        out[...] = jnp.where(first, full[one : one + HALF, :], full[two : two + HALF, :])


def first_kernel(core_ref, basis_hbm, pix_hbm, band_hbm, mag_hbm, var_hbm, mine_ref, other_ref, counts_ref, high_ref, low_ref,
                 raw, pix_ref, band_ref, mag_ref, var_ref, left, right, full, sems, obj_sems):
    obj_copies = [
        pltpu.make_async_copy(src, dst, obj_sems.at[i])
        for i, (src, dst) in enumerate(((pix_hbm, pix_ref), (band_hbm, band_ref), (mag_hbm, mag_ref), (var_hbm, var_ref)))
    ]
    copies = [
        pltpu.make_async_copy(basis_hbm.at[:, pl.ds(i * LANES, LANES)], raw.at[:, pl.ds(i * LANES, LANES)], sems.at[i])
        for i in range(STRIPES)
    ]
    for copy in obj_copies + copies:
        copy.start()
    group_no = lax.broadcasted_iota(jnp.int32, (32, LANES), 0)
    lane_no = lax.broadcasted_iota(jnp.int32, (LANES, LANES), 0)

    for copy in obj_copies:
        copy.wait()

    def objects(block, carry):
        at = pl.multiple_of(block * 8, 8)
        pix = pix_ref[pl.ds(at, 8), :]
        band = band_ref[pl.ds(at, 8), :]
        var = var_ref[pl.ds(at, 8), :]
        weight = var * mag_ref[pl.ds(at, 8), :]
        group = lax.shift_right_logical(pix, 7) * 8 + band
        low_pix = lax.bitwise_and(pix, LANES - 1)
        values = []
        for v in (var, weight):
            high = v.astype(BF16).astype(F32)
            values += [high, v - high]
        for i in range(8):
            mine = group_no == group[i : i + 1, :]
            to = pl.ds(pl.multiple_of(block * 8 * LANES, 8 * LANES) + i * LANES, LANES)
            for k, v in enumerate(values):
                left[k * 32 : (k + 1) * 32, to] = jnp.where(mine, v[i : i + 1, :], 0.0).astype(BF16)
            right[:, to] = jnp.where(lane_no == low_pix[i : i + 1, :], 1.0, 0.0).astype(BF16)
        return carry

    lax.fori_loop(0, OBJ_ROWS // 8, objects, 0)
    sums = dot(left[...], right[...], NT)
    counts, weighted = [
        jnp.concatenate([sums[q + h * 8 : q + h * 8 + 8] + sums[q + 32 + h * 8 : q + 40 + h * 8] for h in range(4)], axis=1)
        for q in (0, 64)
    ]
    counts_ref[...] = counts
    edge = NCOEF // 16 * 16
    for i, copy in enumerate(copies):
        copy.wait()
        cols = pl.ds(i * LANES, LANES)
        for row in range(0, edge, 160):
            rows = pl.ds(row, 160)
            high_ref[rows, cols], low_ref[rows, cols] = split(raw[rows, cols])
        tail = jnp.broadcast_to(raw[edge:NCOEF, cols], (WIDE - edge, LANES))
        tail = jnp.where(lax.broadcasted_iota(jnp.int32, tail.shape, 0) == 0, tail, 0.0)
        high_ref[edge:, cols], low_ref[edge:, cols] = split(tail)
    image_of(weighted, high_ref, low_ref, core_ref, full, mine_ref, other_ref)


def model_and_image(direction, wide, counts_ref, high_ref, low_ref, core_ref, full, mine_ref, other_ref):
    wide[...] = jnp.zeros_like(wide)
    for j in range(TILES):
        wide[:BANDS, j * LANES : (j + 1) * LANES] = direction[j * BANDS : (j + 1) * BANDS, :]
    both = jnp.concatenate(split(wide[...]), axis=0)
    model = dot(both, high_ref[...], NN) + dot(both, low_ref[...], NN)
    image_of(counts_ref[...] * (model[:8] + model[8:]), high_ref, low_ref, core_ref, full, mine_ref, other_ref)


def joined(core_ref, own_ref, near_ref):
    first = core_ref[0:1, :] == 0
    own, near = own_ref[...], near_ref[...]
    return jnp.concatenate([jnp.where(first, own, near), jnp.where(first, near, own)], axis=0)


def total_of(x):
    return jnp.sum(x, keepdims=True)


def start_kernel(root, core_ref, own, near, counts_ref, high_ref, low_ref,
                 mine_ref, other_ref, res_ref, norm_ref, wide, full):
    right_side = joined(core_ref, own, near) / root
    res_ref[...] = right_side
    norm_ref[...] = jnp.broadcast_to(total_of(right_side * right_side), (8, LANES))
    model_and_image(right_side, wide, counts_ref, high_ref, low_ref, core_ref, full, mine_ref, other_ref)


def advance(pixels, whole, sol, res, direction, norm):
    image = whole / pixels + RIDGE * direction
    step = norm / total_of(direction * image)
    sol = sol + step * direction
    res = res - step * image
    norm_next = total_of(res * res)
    return sol, res, res + norm_next / norm * direction, norm_next


def step_kernel(pixels, core_ref, own, near, sol_ref, res_ref, dir_ref, norm_ref, counts_ref, high_ref, low_ref,
                mine_ref, other_ref, sol_out, res_out, dir_out, norm_out, wide, full):
    sol, res, direction, norm = advance(
        pixels, joined(core_ref, own, near), sol_ref[...], res_ref[...], dir_ref[...], norm_ref[0:1, 0:1]
    )
    sol_out[...] = sol
    res_out[...] = res
    dir_out[...] = direction
    norm_out[...] = jnp.broadcast_to(norm, (8, LANES))
    model_and_image(direction, wide, counts_ref, high_ref, low_ref, core_ref, full, mine_ref, other_ref)


def last_kernel(pixels, core_ref, own, near, sol_ref, res_ref, dir_ref, norm_ref, sol_out, res_out):
    sol, res, _, _ = advance(
        pixels, joined(core_ref, own, near), sol_ref[...], res_ref[...], dir_ref[...], norm_ref[0:1, 0:1]
    )
    for value, out in ((sol, sol_out), (res, res_out)):
        for j in range(TILES):
            width = min(LANES, NCOEF - j * LANES)
            out[:, j * LANES : j * LANES + width] = value[j * BANDS : (j + 1) * BANDS, :width]


VMEM = pl.BlockSpec(memory_space=pltpu.VMEM)
HBM = pl.BlockSpec(memory_space=pltpu.HBM)
LIMIT = 24 * 1024 * 1024


def shape(*dims, kind=F32):
    return jax.ShapeDtypeStruct(dims, kind)


def call(kernel, name, outs, ins, scratch=(), limit=LIMIT):
    return pl.pallas_call(
        kernel,
        name=name,
        out_shape=outs,
        in_specs=ins,
        out_specs=[VMEM] * len(outs),
        scratch_shapes=list(scratch),
        compiler_params=pltpu.CompilerParams(vmem_limit_bytes=limit),
    )


def sum_up(parts):
    total = parts[0]
    for i in range(1, parts.shape[0]):
        total = total + parts[i]
    return total


def device(y, z, x, c):
    return ((y * SPAN["z"] + z) * SPAN["x"] + x) * SPAN["c"] + c


def two_rounds():
    ys, zs, xs, pairs = range(SPAN["y"]), range(SPAN["z"]), range(SPAN["x"]), range(SPAN["y"] // 2)
    spread = sorted(zs, key=lambda z: (z % 2, z // 2 % 2, z))
    one = [[device(y, z, x, 0) for y in ys for x in xs] for z in zs]
    one += [[device(2 * pair + k, z, x, 1) for z in zs for k in (0, 1)] for x in xs for pair in pairs]
    two = [[device(y, z, x, 0) for z in spread] for y in ys for x in xs]
    two += [[device(y, z, x, 1) for x in xs for y in take] for z in zs for take in ((0, 3), (1, 2))]
    return one, two


def sent_to_all(block, groups):
    size = len(groups[0])
    sent = jnp.broadcast_to(block[None], (size, *block.shape))
    return sum_up(lax.all_to_all(sent, AXES, 0, 0, tiled=True, axis_index_groups=groups))


def summed(mine, other):
    swap = [(0, 1), (1, 0)]
    mine = mine + lax.ppermute(other, "c", swap)
    for groups in two_rounds():
        mine = sent_to_all(mine, groups)
    return mine, lax.ppermute(mine, "c", swap)


def body(basis, pixel_ids, band_ids, mags, inv_var):
    pixels = float(PIX * 256)
    objects = [a.reshape(OBJ_ROWS, LANES) for a in (pixel_ids, band_ids, mags, inv_var)]
    core = jnp.broadcast_to(lax.axis_index("c"), (8, LANES)).astype(jnp.int32)
    vec, half, norm_shape = shape(ROWS, LANES), shape(HALF, LANES), shape(8, LANES)
    scratch = [pltpu.VMEM((8, WIDE), F32), pltpu.VMEM((ROWS, LANES), F32)]
    copied = shape(WIDE, PIX, kind=BF16)
    mine, other, counts, high, low = call(
        first_kernel,
        "first",
        [half, half, shape(8, PIX), copied, copied],
        [VMEM] + [HBM] * 5,
        [
            pltpu.VMEM((NCOEF, PIX), F32),
            pltpu.VMEM((OBJ_ROWS, LANES), jnp.int32),
            pltpu.VMEM((OBJ_ROWS, LANES), jnp.int32),
            pltpu.VMEM((OBJ_ROWS, LANES), F32),
            pltpu.VMEM((OBJ_ROWS, LANES), F32),
            pltpu.VMEM((128, OBJ_ROWS * LANES), BF16),
            pltpu.VMEM((128, OBJ_ROWS * LANES), BF16),
            pltpu.VMEM((ROWS, LANES), F32),
            pltpu.SemaphoreType.DMA((STRIPES,)),
            pltpu.SemaphoreType.DMA((4,)),
        ],
    )(core, *[pltpu.with_memory_space_constraint(a, pltpu.HBM) for a in (basis.T, *objects)])
    mine, other, res, norm = call(
        functools.partial(start_kernel, pixels**0.5), "start", [half, half, vec, norm_shape], [VMEM] * 6, scratch
    )(core, *summed(mine, other), counts, high, low)
    sol, direction = jnp.zeros((ROWS, LANES), F32), res
    for _ in range(ITERS - 1):
        mine, other, sol, res, direction, norm = call(
            functools.partial(step_kernel, pixels), "step", [half, half, vec, vec, vec, norm_shape], [VMEM] * 10, scratch
        )(core, *summed(mine, other), sol, res, direction, norm, counts, high, low)
    out = shape(BANDS, NCOEF)
    return tuple(
        call(functools.partial(last_kernel, pixels), "last", [out, out], [VMEM] * 7)(
            core, *summed(mine, other), sol, res, direction, norm
        )
    )


def solution(mesh):
    torus = Mesh(mesh.devices.reshape(*(SPAN[a] for a in AXES)), AXES)
    return jax.shard_map(
        body,
        mesh=torus,
        in_specs=(P(AXES, None),) + (P(AXES),) * 4,
        out_specs=(P(), P()),
        check_vma=False,
    )
```

```python
import functools

import jax
import jax.numpy as jnp
from jax import lax
from jax.experimental import pallas as pl
from jax.experimental.pallas import tpu as pltpu
from jax.sharding import Mesh
from jax.sharding import PartitionSpec as P

BANDS = 5
ITERS = 3
AXES = ("y", "z", "x", "c")
SPAN = {"y": 4, "z": 8, "x": 4, "c": 2}
RIDGE = 0.1
PIX = 512
NCOEF = 2401
LANES = 128
TILES = -(-NCOEF // LANES)
WIDE = TILES * LANES
ROWS = 96
HALF = ROWS // 2
OBJ_ROWS = 64
STRIPES = PIX // LANES
NT = (((1,), (1,)), ((), ()))
NN = (((1,), (0,)), ((), ()))
F32, BF16 = jnp.float32, jnp.bfloat16


def dot(a, b, dims):
    return lax.dot_general(a, b, dims, preferred_element_type=F32)


def split(x):
    high = x.astype(BF16)
    return high, (x - high.astype(F32)).astype(BF16)


def image_of(scaled, high_turned, low_turned, core_ref, full, mine_ref, other_ref):
    both = jnp.concatenate(split(scaled), axis=0)
    total = dot(both, high_turned[...], NN) + dot(both, low_turned[...], NN)
    total = total[:8] + total[8:]
    for j in range(TILES):
        full[j * BANDS : (j + 1) * BANDS, :] = total[:BANDS, j * LANES : (j + 1) * LANES]
    full[TILES * BANDS :, :] = jnp.zeros((ROWS - TILES * BANDS, LANES), F32)
    first = core_ref[0:1, :] == 0
    for out, one, two in ((mine_ref, 0, HALF), (other_ref, HALF, 0)):
        out[...] = jnp.where(first, full[one : one + HALF, :], full[two : two + HALF, :])


def first_kernel(core_ref, basis_hbm, pix_hbm, band_hbm, mag_hbm, var_hbm, mine_ref, other_ref, counts_ref, high_ref, low_ref, high_turned, low_turned,
                 raw, pix_ref, band_ref, mag_ref, var_ref, left, right, full, sems, obj_sems):
    obj_copies = [
        pltpu.make_async_copy(src, dst, obj_sems.at[i])
        for i, (src, dst) in enumerate(((pix_hbm, pix_ref), (band_hbm, band_ref), (mag_hbm, mag_ref), (var_hbm, var_ref)))
    ]
    copies = [
        pltpu.make_async_copy(basis_hbm.at[:, pl.ds(i * LANES, LANES)], raw.at[:, pl.ds(i * LANES, LANES)], sems.at[i])
        for i in range(STRIPES)
    ]
    for copy in obj_copies + copies:
        copy.start()
    group_no = lax.broadcasted_iota(jnp.int32, (32, LANES), 0)
    lane_no = lax.broadcasted_iota(jnp.int32, (LANES, LANES), 0)

    for copy in obj_copies:
        copy.wait()

    def objects(block, carry):
        at = pl.multiple_of(block * 8, 8)
        pix = pix_ref[pl.ds(at, 8), :]
        band = band_ref[pl.ds(at, 8), :]
        var = var_ref[pl.ds(at, 8), :]
        weight = var * mag_ref[pl.ds(at, 8), :]
        group = lax.shift_right_logical(pix, 7) * 8 + band
        low_pix = lax.bitwise_and(pix, LANES - 1)
        values = []
        for v in (var, weight):
            high = v.astype(BF16).astype(F32)
            values += [high, v - high]
        for i in range(8):
            mine = group_no == group[i : i + 1, :]
            to = pl.ds(pl.multiple_of(block * 8 * LANES, 8 * LANES) + i * LANES, LANES)
            for k, v in enumerate(values):
                left[k * 32 : (k + 1) * 32, to] = jnp.where(mine, v[i : i + 1, :], 0.0).astype(BF16)
            right[:, to] = jnp.where(lane_no == low_pix[i : i + 1, :], 1.0, 0.0).astype(BF16)
        return carry

    lax.fori_loop(0, OBJ_ROWS // 8, objects, 0)
    sums = dot(left[...], right[...], NT)
    counts, weighted = [
        jnp.concatenate([sums[q + h * 8 : q + h * 8 + 8] + sums[q + 32 + h * 8 : q + 40 + h * 8] for h in range(4)], axis=1)
        for q in (0, 64)
    ]
    counts_ref[...] = counts
    edge = NCOEF // 16 * 16
    for i, copy in enumerate(copies):
        copy.wait()
        cols = pl.ds(i * LANES, LANES)
        for j in range(TILES):
            rows = pl.ds(j * LANES, LANES)
            if j < TILES - 1:
                block = raw[rows, cols]
            else:
                size = WIDE - edge
                tail = jnp.broadcast_to(raw[edge:NCOEF, cols], (size, LANES))
                tail = jnp.where(lax.broadcasted_iota(jnp.int32, tail.shape, 0) == 0, tail, 0.0)
                block = jnp.concatenate([raw[j * LANES : edge, cols], tail], axis=0)
            high, low = split(block)
            high_ref[rows, cols], low_ref[rows, cols] = high, low
            high_turned[cols, rows], low_turned[cols, rows] = high.T, low.T
    image_of(weighted, high_turned, low_turned, core_ref, full, mine_ref, other_ref)


def model_and_image(direction, wide, counts_ref, high_ref, low_ref, high_turned, low_turned, core_ref, full, mine_ref, other_ref):
    wide[...] = jnp.zeros_like(wide)
    for j in range(TILES):
        wide[:BANDS, j * LANES : (j + 1) * LANES] = direction[j * BANDS : (j + 1) * BANDS, :]
    both = jnp.concatenate(split(wide[...]), axis=0)
    model = dot(both, high_ref[...], NN) + dot(both, low_ref[...], NN)
    image_of(counts_ref[...] * (model[:8] + model[8:]), high_turned, low_turned, core_ref, full, mine_ref, other_ref)


def joined(core_ref, own_ref, near_ref):
    first = core_ref[0:1, :] == 0
    own, near = own_ref[...], near_ref[...]
    return jnp.concatenate([jnp.where(first, own, near), jnp.where(first, near, own)], axis=0)


def total_of(x):
    return jnp.sum(x, keepdims=True)


def start_kernel(root, core_ref, own, near, counts_ref, high_ref, low_ref, high_turned, low_turned,
                 mine_ref, other_ref, res_ref, norm_ref, wide, full):
    right_side = joined(core_ref, own, near) / root
    res_ref[...] = right_side
    norm_ref[...] = jnp.broadcast_to(total_of(right_side * right_side), (8, LANES))
    model_and_image(right_side, wide, counts_ref, high_ref, low_ref, high_turned, low_turned, core_ref, full, mine_ref, other_ref)


def advance(pixels, whole, sol, res, direction, norm):
    image = whole / pixels + RIDGE * direction
    step = norm / total_of(direction * image)
    sol = sol + step * direction
    res = res - step * image
    norm_next = total_of(res * res)
    return sol, res, res + norm_next / norm * direction, norm_next


def step_kernel(pixels, core_ref, own, near, sol_ref, res_ref, dir_ref, norm_ref, counts_ref, high_ref, low_ref, high_turned, low_turned,
                mine_ref, other_ref, sol_out, res_out, dir_out, norm_out, wide, full):
    sol, res, direction, norm = advance(
        pixels, joined(core_ref, own, near), sol_ref[...], res_ref[...], dir_ref[...], norm_ref[0:1, 0:1]
    )
    sol_out[...] = sol
    res_out[...] = res
    dir_out[...] = direction
    norm_out[...] = jnp.broadcast_to(norm, (8, LANES))
    model_and_image(direction, wide, counts_ref, high_ref, low_ref, high_turned, low_turned, core_ref, full, mine_ref, other_ref)


def last_kernel(pixels, core_ref, own, near, sol_ref, res_ref, dir_ref, norm_ref, sol_out, res_out):
    sol, res, _, _ = advance(
        pixels, joined(core_ref, own, near), sol_ref[...], res_ref[...], dir_ref[...], norm_ref[0:1, 0:1]
    )
    for value, out in ((sol, sol_out), (res, res_out)):
        for j in range(TILES):
            width = min(LANES, NCOEF - j * LANES)
            out[:, j * LANES : j * LANES + width] = value[j * BANDS : (j + 1) * BANDS, :width]


VMEM = pl.BlockSpec(memory_space=pltpu.VMEM)
HBM = pl.BlockSpec(memory_space=pltpu.HBM)
LIMIT = 24 * 1024 * 1024


def shape(*dims, kind=F32):
    return jax.ShapeDtypeStruct(dims, kind)


def call(kernel, name, outs, ins, scratch=(), limit=LIMIT):
    return pl.pallas_call(
        kernel,
        name=name,
        out_shape=outs,
        in_specs=ins,
        out_specs=[VMEM] * len(outs),
        scratch_shapes=list(scratch),
        compiler_params=pltpu.CompilerParams(vmem_limit_bytes=limit),
    )


def sum_up(parts):
    total = parts[0]
    for i in range(1, parts.shape[0]):
        total = total + parts[i]
    return total


def device(y, z, x, c):
    return ((y * SPAN["z"] + z) * SPAN["x"] + x) * SPAN["c"] + c


def two_rounds():
    ys, zs, xs, pairs = range(SPAN["y"]), range(SPAN["z"]), range(SPAN["x"]), range(SPAN["y"] // 2)
    spread = sorted(zs, key=lambda z: (z % 2, z // 2 % 2, z))
    halves = sorted(xs, key=lambda x: (x % 2, x))
    one = [[device(y, z, x, 0) for y in halves for x in halves] for z in zs]
    one += [[device(2 * pair + k, z, x, 1) for z in zs for k in (0, 1)] for x in xs for pair in pairs]
    two = [[device(y, z, x, 0) for z in spread] for y in ys for x in xs]
    two += [[device(y, z, x, 1) for x in xs for y in take] for z in zs for take in ((0, 3), (1, 2))]
    return one, two


def sent_to_all(block, groups):
    size = len(groups[0])
    sent = jnp.broadcast_to(block[None], (size, *block.shape))
    return sum_up(lax.all_to_all(sent, AXES, 0, 0, tiled=True, axis_index_groups=groups))


def summed(mine, other):
    swap = [(0, 1), (1, 0)]
    mine = mine + lax.ppermute(other, "c", swap)
    for groups in two_rounds():
        mine = sent_to_all(mine, groups)
    return mine, lax.ppermute(mine, "c", swap)


def body(basis, pixel_ids, band_ids, mags, inv_var):
    pixels = float(PIX * 256)
    objects = [a.reshape(OBJ_ROWS, LANES) for a in (pixel_ids, band_ids, mags, inv_var)]
    core = jnp.broadcast_to(lax.axis_index("c"), (8, LANES)).astype(jnp.int32)
    vec, half, norm_shape = shape(ROWS, LANES), shape(HALF, LANES), shape(8, LANES)
    scratch = [pltpu.VMEM((8, WIDE), F32), pltpu.VMEM((ROWS, LANES), F32)]
    copied, turned = shape(WIDE, PIX, kind=BF16), shape(PIX, WIDE, kind=BF16)
    mine, other, *fixed = call(
        first_kernel,
        "first",
        [half, half, shape(8, PIX), copied, copied, turned, turned],
        [VMEM] + [HBM] * 5,
        [
            pltpu.VMEM((NCOEF, PIX), F32),
            pltpu.VMEM((OBJ_ROWS, LANES), jnp.int32),
            pltpu.VMEM((OBJ_ROWS, LANES), jnp.int32),
            pltpu.VMEM((OBJ_ROWS, LANES), F32),
            pltpu.VMEM((OBJ_ROWS, LANES), F32),
            pltpu.VMEM((128, OBJ_ROWS * LANES), BF16),
            pltpu.VMEM((128, OBJ_ROWS * LANES), BF16),
            pltpu.VMEM((ROWS, LANES), F32),
            pltpu.SemaphoreType.DMA((STRIPES,)),
            pltpu.SemaphoreType.DMA((4,)),
        ],
    )(core, *[pltpu.with_memory_space_constraint(a, pltpu.HBM) for a in (basis.T, *objects)])
    mine, other, res, norm = call(
        functools.partial(start_kernel, pixels**0.5), "start", [half, half, vec, norm_shape], [VMEM] * 8, scratch
    )(core, *summed(mine, other), *fixed)
    sol, direction = jnp.zeros((ROWS, LANES), F32), res
    for _ in range(ITERS - 1):
        mine, other, sol, res, direction, norm = call(
            functools.partial(step_kernel, pixels), "step", [half, half, vec, vec, vec, norm_shape], [VMEM] * 12, scratch
        )(core, *summed(mine, other), sol, res, direction, norm, *fixed)
    out = shape(BANDS, NCOEF)
    return tuple(
        call(functools.partial(last_kernel, pixels), "last", [out, out], [VMEM] * 7)(
            core, *summed(mine, other), sol, res, direction, norm
        )
    )


def solution(mesh):
    torus = Mesh(mesh.devices.reshape(*(SPAN[a] for a in AXES)), AXES)
    return jax.shard_map(
        body,
        mesh=torus,
        in_specs=(P(AXES, None),) + (P(AXES),) * 4,
        out_specs=(P(), P()),
        check_vma=False,
    )
```

```python
import functools

import jax
import jax.numpy as jnp
from jax import lax
from jax.experimental import pallas as pl
from jax.experimental.pallas import tpu as pltpu
from jax.sharding import Mesh
from jax.sharding import PartitionSpec as P

BANDS = 5
ITERS = 3
AXES = ("y", "z", "x", "c")
SPAN = {"y": 4, "z": 8, "x": 4, "c": 2}
RIDGE = 0.1
PIX = 512
NCOEF = 2401
LANES = 128
TILES = -(-NCOEF // LANES)
WIDE = TILES * LANES
ROWS = 96
HALF = ROWS // 2
OBJ_ROWS = 64
NT = (((1,), (1,)), ((), ()))
NN = (((1,), (0,)), ((), ()))
F32, BF16 = jnp.float32, jnp.bfloat16


def dot(a, b, dims):
    return lax.dot_general(a, b, dims, preferred_element_type=F32)


def split(x):
    high = x.astype(BF16)
    return high, (x - high.astype(F32)).astype(BF16)


def image_of(scaled, high_turned, low_turned, core_ref, full, mine_ref, other_ref):
    both = jnp.concatenate(split(scaled), axis=0)
    total = dot(both, high_turned[...], NN) + dot(both, low_turned[...], NN)
    total = total[:8] + total[8:]
    for j in range(TILES):
        full[j * BANDS : (j + 1) * BANDS, :] = total[:BANDS, j * LANES : (j + 1) * LANES]
    full[TILES * BANDS :, :] = jnp.zeros((ROWS - TILES * BANDS, LANES), F32)
    first = core_ref[0:1, :] == 0
    for out, one, two in ((mine_ref, 0, HALF), (other_ref, HALF, 0)):
        out[...] = jnp.where(first, full[one : one + HALF, :], full[two : two + HALF, :])


def first_kernel(core_ref, basis_hbm, pix_hbm, band_hbm, mag_hbm, var_hbm, mine_ref, other_ref, counts_ref, high_ref, low_ref, high_turned, low_turned,
                 raw, pix_ref, band_ref, mag_ref, var_ref, left, right, full, sem, obj_sems):
    obj_copies = [
        pltpu.make_async_copy(src, dst, obj_sems.at[i])
        for i, (src, dst) in enumerate(((pix_hbm, pix_ref), (band_hbm, band_ref), (mag_hbm, mag_ref), (var_hbm, var_ref)))
    ]
    basis_copy = pltpu.make_async_copy(basis_hbm, raw, sem)
    for copy in (*obj_copies, basis_copy):
        copy.start()
    number = lax.broadcasted_iota(jnp.int32, (LANES, LANES), 0).astype(BF16)
    sixteen = (16, LANES)
    one, zero = jnp.ones(sixteen, BF16), jnp.zeros(sixteen, BF16)
    for copy in obj_copies:
        copy.wait()

    def objects(block, carry):
        at = pl.multiple_of(block * 8, 8)
        pix = pix_ref[pl.ds(at, 8), :]
        band = band_ref[pl.ds(at, 8), :]
        var = var_ref[pl.ds(at, 8), :]
        weight = var * mag_ref[pl.ds(at, 8), :]
        group = (lax.shift_right_logical(pix, 7) * 8 + band).astype(F32)
        low_pix = lax.bitwise_and(pix, LANES - 1).astype(F32)
        values = []
        for v in (var, weight):
            high = v.astype(BF16).astype(F32)
            values += [high, v - high]

        def spread(rows, i):
            return jnp.broadcast_to(rows[i : i + 1, :], sixteen).astype(BF16)

        for i in range(8):
            to = pl.ds(pl.multiple_of(block * 8 * LANES, 8 * LANES) + i * LANES, LANES)
            mine = spread(group, i)
            where = [number[k : k + 16, :] == mine for k in (0, 16)]
            for k, v in enumerate(values):
                v = spread(v, i)
                for h in (0, 1):
                    left[k * 32 + h * 16 : k * 32 + h * 16 + 16, to] = jnp.where(where[h], v, zero)
            pixel = spread(low_pix, i)
            for k in range(0, LANES, 16):
                right[k : k + 16, to] = jnp.where(number[k : k + 16, :] == pixel, one, zero)
        return carry

    lax.fori_loop(0, OBJ_ROWS // 8, objects, 0)
    sums = dot(left[...], right[...], NT)
    counts, weighted = [
        jnp.concatenate([sums[q + h * 8 : q + h * 8 + 8] + sums[q + 32 + h * 8 : q + 40 + h * 8] for h in range(4)], axis=1)
        for q in (0, 64)
    ]
    counts_ref[...] = counts
    edge = NCOEF // 16 * 16
    basis_copy.wait()
    for i in range(PIX // LANES):
        cols = pl.ds(i * LANES, LANES)
        for j in range(TILES):
            rows = pl.ds(j * LANES, LANES)
            if j < TILES - 1:
                block = raw[rows, cols]
            else:
                size = WIDE - edge
                tail = jnp.broadcast_to(raw[edge:NCOEF, cols], (size, LANES))
                tail = jnp.where(lax.broadcasted_iota(jnp.int32, tail.shape, 0) == 0, tail, 0.0)
                block = jnp.concatenate([raw[j * LANES : edge, cols], tail], axis=0)
            high, low = split(block)
            high_ref[rows, cols], low_ref[rows, cols] = high, low
            high_turned[cols, rows], low_turned[cols, rows] = high.T, low.T
    image_of(weighted, high_turned, low_turned, core_ref, full, mine_ref, other_ref)


def model_and_image(direction, wide, counts_ref, high_ref, low_ref, high_turned, low_turned, core_ref, full, mine_ref, other_ref):
    wide[...] = jnp.zeros_like(wide)
    for j in range(TILES):
        wide[:BANDS, j * LANES : (j + 1) * LANES] = direction[j * BANDS : (j + 1) * BANDS, :]
    both = jnp.concatenate(split(wide[...]), axis=0)
    model = dot(both, high_ref[...], NN) + dot(both, low_ref[...], NN)
    image_of(counts_ref[...] * (model[:8] + model[8:]), high_turned, low_turned, core_ref, full, mine_ref, other_ref)


def joined(core_ref, own_ref, near_ref):
    first = core_ref[0:1, :] == 0
    own, near = own_ref[...], near_ref[...]
    return jnp.concatenate([jnp.where(first, own, near), jnp.where(first, near, own)], axis=0)


def total_of(x):
    return jnp.sum(x, keepdims=True)


def start_kernel(root, core_ref, own, near, counts_ref, high_ref, low_ref, high_turned, low_turned,
                 mine_ref, other_ref, res_ref, norm_ref, wide, full):
    right_side = joined(core_ref, own, near) / root
    res_ref[...] = right_side
    norm_ref[...] = jnp.broadcast_to(total_of(right_side * right_side), (8, LANES))
    model_and_image(right_side, wide, counts_ref, high_ref, low_ref, high_turned, low_turned, core_ref, full, mine_ref, other_ref)


def advance(pixels, whole, sol, res, direction, norm):
    image = whole / pixels + RIDGE * direction
    step = norm / total_of(direction * image)
    sol = sol + step * direction
    res = res - step * image
    norm_next = total_of(res * res)
    return sol, res, res + norm_next / norm * direction, norm_next


def step_kernel(pixels, core_ref, own, near, sol_ref, res_ref, dir_ref, norm_ref, counts_ref, high_ref, low_ref, high_turned, low_turned,
                mine_ref, other_ref, sol_out, res_out, dir_out, norm_out, wide, full):
    sol, res, direction, norm = advance(
        pixels, joined(core_ref, own, near), sol_ref[...], res_ref[...], dir_ref[...], norm_ref[0:1, 0:1]
    )
    sol_out[...] = sol
    res_out[...] = res
    dir_out[...] = direction
    norm_out[...] = jnp.broadcast_to(norm, (8, LANES))
    model_and_image(direction, wide, counts_ref, high_ref, low_ref, high_turned, low_turned, core_ref, full, mine_ref, other_ref)


def last_kernel(pixels, core_ref, own, near, sol_ref, res_ref, dir_ref, norm_ref, sol_out, res_out):
    sol, res, _, _ = advance(
        pixels, joined(core_ref, own, near), sol_ref[...], res_ref[...], dir_ref[...], norm_ref[0:1, 0:1]
    )
    for value, out in ((sol, sol_out), (res, res_out)):
        for j in range(TILES):
            width = min(LANES, NCOEF - j * LANES)
            out[:, j * LANES : j * LANES + width] = value[j * BANDS : (j + 1) * BANDS, :width]


VMEM = pl.BlockSpec(memory_space=pltpu.VMEM)
HBM = pl.BlockSpec(memory_space=pltpu.HBM)
LIMIT = 24 * 1024 * 1024


def shape(*dims, kind=F32):
    return jax.ShapeDtypeStruct(dims, kind)


def call(kernel, name, outs, ins, scratch=(), limit=LIMIT):
    return pl.pallas_call(
        kernel,
        name=name,
        out_shape=outs,
        in_specs=ins,
        out_specs=[VMEM] * len(outs),
        scratch_shapes=list(scratch),
        compiler_params=pltpu.CompilerParams(vmem_limit_bytes=limit),
    )


def sum_up(parts):
    total = parts[0]
    for i in range(1, parts.shape[0]):
        total = total + parts[i]
    return total


def device(y, z, x, c):
    return ((y * SPAN["z"] + z) * SPAN["x"] + x) * SPAN["c"] + c


def two_rounds():
    ys, zs, xs, pairs = range(SPAN["y"]), range(SPAN["z"]), range(SPAN["x"]), range(SPAN["y"] // 2)
    spread = sorted(zs, key=lambda z: (z % 2, z // 2 % 2, z))
    halves = sorted(xs, key=lambda x: (x % 2, x))
    one = [[device(y, z, x, 0) for y in halves for x in halves] for z in zs]
    one += [[device(2 * pair + k, z, x, 1) for z in zs for k in (0, 1)] for x in xs for pair in pairs]
    two = [[device(y, z, x, 0) for z in spread] for y in ys for x in xs]
    two += [[device(y, z, x, 1) for x in xs for y in take] for z in zs for take in ((0, 3), (1, 2))]
    return one, two


def sent_to_all(block, groups):
    size = len(groups[0])
    sent = jnp.broadcast_to(block[None], (size, *block.shape))
    return sum_up(lax.all_to_all(sent, AXES, 0, 0, tiled=True, axis_index_groups=groups))


def summed(mine, other):
    swap = [(0, 1), (1, 0)]
    mine = mine + lax.ppermute(other, "c", swap)
    for groups in two_rounds():
        mine = sent_to_all(mine, groups)
    return mine, lax.ppermute(mine, "c", swap)


def body(basis, pixel_ids, band_ids, mags, inv_var):
    pixels = float(PIX * 256)
    objects = [a.reshape(OBJ_ROWS, LANES) for a in (pixel_ids, band_ids, mags, inv_var)]
    core = jnp.broadcast_to(lax.axis_index("c"), (8, LANES)).astype(jnp.int32)
    vec, half, norm_shape = shape(ROWS, LANES), shape(HALF, LANES), shape(8, LANES)
    scratch = [pltpu.VMEM((8, WIDE), F32), pltpu.VMEM((ROWS, LANES), F32)]
    copied, turned = shape(WIDE, PIX, kind=BF16), shape(PIX, WIDE, kind=BF16)
    mine, other, *fixed = call(
        first_kernel,
        "first",
        [half, half, shape(8, PIX), copied, copied, turned, turned],
        [VMEM] + [HBM] * 5,
        [
            pltpu.VMEM((NCOEF, PIX), F32),
            pltpu.VMEM((OBJ_ROWS, LANES), jnp.int32),
            pltpu.VMEM((OBJ_ROWS, LANES), jnp.int32),
            pltpu.VMEM((OBJ_ROWS, LANES), F32),
            pltpu.VMEM((OBJ_ROWS, LANES), F32),
            pltpu.VMEM((128, OBJ_ROWS * LANES), BF16),
            pltpu.VMEM((128, OBJ_ROWS * LANES), BF16),
            pltpu.VMEM((ROWS, LANES), F32),
            pltpu.SemaphoreType.DMA,
            pltpu.SemaphoreType.DMA((4,)),
        ],
    )(core, *[pltpu.with_memory_space_constraint(a, pltpu.HBM) for a in (basis.T, *objects)])
    mine, other, res, norm = call(
        functools.partial(start_kernel, pixels**0.5), "start", [half, half, vec, norm_shape], [VMEM] * 8, scratch
    )(core, *summed(mine, other), *fixed)
    sol, direction = jnp.zeros((ROWS, LANES), F32), res
    for _ in range(ITERS - 1):
        mine, other, sol, res, direction, norm = call(
            functools.partial(step_kernel, pixels), "step", [half, half, vec, vec, vec, norm_shape], [VMEM] * 12, scratch
        )(core, *summed(mine, other), sol, res, direction, norm, *fixed)
    out = shape(BANDS, NCOEF)
    return tuple(
        call(functools.partial(last_kernel, pixels), "last", [out, out], [VMEM] * 7)(
            core, *summed(mine, other), sol, res, direction, norm
        )
    )


def solution(mesh):
    torus = Mesh(mesh.devices.reshape(*(SPAN[a] for a in AXES)), AXES)
    return jax.shard_map(
        body,
        mesh=torus,
        in_specs=(P(AXES, None),) + (P(AXES),) * 4,
        out_specs=(P(), P()),
        check_vma=False,
    )
```

```python
import functools

import jax
import jax.numpy as jnp
from jax import lax
from jax.experimental import pallas as pl
from jax.experimental.pallas import tpu as pltpu
from jax.sharding import Mesh
from jax.sharding import PartitionSpec as P

BANDS = 5
ITERS = 3
AXES = ("y", "z", "x", "c")
SPAN = {"y": 4, "z": 8, "x": 4, "c": 2}
RIDGE = 0.1
PIX = 512
NCOEF = 2401
LANES = 128
TILES = -(-NCOEF // LANES)
WIDE = TILES * LANES
ROWS = 96
HALF = ROWS // 2
OBJ_ROWS = 64
NT = (((1,), (1,)), ((), ()))
NN = (((1,), (0,)), ((), ()))
F32, BF16 = jnp.float32, jnp.bfloat16


def dot(a, b, dims):
    return lax.dot_general(a, b, dims, preferred_element_type=F32)


def split(x):
    high = x.astype(BF16)
    return high, (x - high.astype(F32)).astype(BF16)


def image_of(scaled, high_turned, low_turned, core_ref, full, mine_ref, other_ref):
    both = jnp.concatenate(split(scaled), axis=0)
    total = dot(both, high_turned[...], NN) + dot(both, low_turned[...], NN)
    total = total[:8] + total[8:]
    for j in range(TILES):
        full[j * BANDS : (j + 1) * BANDS, :] = total[:BANDS, j * LANES : (j + 1) * LANES]
    full[TILES * BANDS :, :] = jnp.zeros((ROWS - TILES * BANDS, LANES), F32)
    first = core_ref[0:1, :] == 0
    for out, one, two in ((mine_ref, 0, HALF), (other_ref, HALF, 0)):
        out[...] = jnp.where(first, full[one : one + HALF, :], full[two : two + HALF, :])


def first_kernel(core_ref, basis_hbm, pix_hbm, band_hbm, mag_hbm, var_hbm, mine_ref, other_ref, counts_ref, high_ref, low_ref, high_turned, low_turned,
                 raw, pix_ref, band_ref, mag_ref, var_ref, left, right, full, sem, obj_sems):
    obj_copies = [
        pltpu.make_async_copy(src, dst, obj_sems.at[i])
        for i, (src, dst) in enumerate(((pix_hbm, pix_ref), (band_hbm, band_ref), (mag_hbm, mag_ref), (var_hbm, var_ref)))
    ]
    basis_copy = pltpu.make_async_copy(basis_hbm, raw, sem)
    for copy in (*obj_copies, basis_copy):
        copy.start()
    number = lax.broadcasted_iota(jnp.int32, (LANES, LANES), 0).astype(BF16)
    sixteen = (16, LANES)
    one, zero = jnp.ones(sixteen, BF16), jnp.zeros(sixteen, BF16)
    for copy in obj_copies:
        copy.wait()

    def objects(block, carry):
        at = pl.multiple_of(block * 8, 8)
        pix = pix_ref[pl.ds(at, 8), :]
        band = band_ref[pl.ds(at, 8), :]
        var = var_ref[pl.ds(at, 8), :]
        weight = var * mag_ref[pl.ds(at, 8), :]
        group = (lax.shift_right_logical(pix, 7) * 8 + band).astype(F32)
        low_pix = lax.bitwise_and(pix, LANES - 1).astype(F32)
        values = []
        for v in (var, weight):
            high = v.astype(BF16).astype(F32)
            values += [high, v - high]

        def spread(rows, i):
            return jnp.broadcast_to(rows[i : i + 1, :], sixteen).astype(BF16)

        for i in range(8):
            to = pl.ds(pl.multiple_of(block * 8 * LANES, 8 * LANES) + i * LANES, LANES)
            mine = spread(group, i)
            where = [number[k : k + 16, :] == mine for k in (0, 16)]
            for k, v in enumerate(values):
                v = spread(v, i)
                for h in (0, 1):
                    left[k * 32 + h * 16 : k * 32 + h * 16 + 16, to] = jnp.where(where[h], v, zero)
            pixel = spread(low_pix, i)
            for k in range(0, LANES, 16):
                right[k : k + 16, to] = jnp.where(number[k : k + 16, :] == pixel, one, zero)
        return carry

    lax.fori_loop(0, OBJ_ROWS // 8, objects, 0)
    sums = dot(left[...], right[...], NT)
    counts, weighted = [
        jnp.concatenate([sums[q + h * 8 : q + h * 8 + 8] + sums[q + 32 + h * 8 : q + 40 + h * 8] for h in range(4)], axis=1)
        for q in (0, 64)
    ]
    counts_ref[...] = counts
    edge = NCOEF // 16 * 16
    basis_copy.wait()
    for i in range(PIX // LANES):
        cols = pl.ds(i * LANES, LANES)
        for j in range(TILES):
            rows = pl.ds(j * LANES, LANES)
            if j < TILES - 1:
                block = raw[rows, cols]
            else:
                size = WIDE - edge
                tail = jnp.broadcast_to(raw[edge:NCOEF, cols], (size, LANES))
                tail = jnp.where(lax.broadcasted_iota(jnp.int32, tail.shape, 0) == 0, tail, 0.0)
                block = jnp.concatenate([raw[j * LANES : edge, cols], tail], axis=0)
            high, low = split(block)
            high_ref[rows, cols], low_ref[rows, cols] = high, low
            high_turned[cols, rows], low_turned[cols, rows] = high.T, low.T
    image_of(weighted, high_turned, low_turned, core_ref, full, mine_ref, other_ref)


def model_and_image(direction, wide, counts_ref, high_ref, low_ref, high_turned, low_turned, core_ref, full, mine_ref, other_ref):
    wide[...] = jnp.zeros_like(wide)
    for j in range(TILES):
        wide[:BANDS, j * LANES : (j + 1) * LANES] = direction[j * BANDS : (j + 1) * BANDS, :]
    both = jnp.concatenate(split(wide[...]), axis=0)
    model = dot(both, high_ref[...], NN) + dot(both, low_ref[...], NN)
    image_of(counts_ref[...] * (model[:8] + model[8:]), high_turned, low_turned, core_ref, full, mine_ref, other_ref)


def joined(core_ref, own_ref, near_ref):
    first = core_ref[0:1, :] == 0
    own, near = own_ref[...], near_ref[...]
    return jnp.concatenate([jnp.where(first, own, near), jnp.where(first, near, own)], axis=0)


def total_of(x):
    return jnp.sum(x, keepdims=True)


def start_kernel(root, core_ref, own, near, counts_ref, high_ref, low_ref, high_turned, low_turned,
                 mine_ref, other_ref, res_ref, norm_ref, wide, full):
    right_side = joined(core_ref, own, near) / root
    res_ref[...] = right_side
    norm_ref[...] = jnp.broadcast_to(total_of(right_side * right_side), (8, LANES))
    model_and_image(right_side, wide, counts_ref, high_ref, low_ref, high_turned, low_turned, core_ref, full, mine_ref, other_ref)


def advance(pixels, whole, sol, res, direction, norm):
    image = whole / pixels + RIDGE * direction
    step = norm / total_of(direction * image)
    sol = sol + step * direction
    res = res - step * image
    norm_next = total_of(res * res)
    return sol, res, res + norm_next / norm * direction, norm_next


def step_kernel(pixels, core_ref, own, near, sol_ref, res_ref, dir_ref, norm_ref, counts_ref, high_ref, low_ref, high_turned, low_turned,
                mine_ref, other_ref, sol_out, res_out, dir_out, norm_out, wide, full):
    sol, res, direction, norm = advance(
        pixels, joined(core_ref, own, near), sol_ref[...], res_ref[...], dir_ref[...], norm_ref[0:1, 0:1]
    )
    sol_out[...] = sol
    res_out[...] = res
    dir_out[...] = direction
    norm_out[...] = jnp.broadcast_to(norm, (8, LANES))
    model_and_image(direction, wide, counts_ref, high_ref, low_ref, high_turned, low_turned, core_ref, full, mine_ref, other_ref)


def last_kernel(pixels, core_ref, own, near, sol_ref, res_ref, dir_ref, norm_ref, sol_out, res_out):
    sol, res, _, _ = advance(
        pixels, joined(core_ref, own, near), sol_ref[...], res_ref[...], dir_ref[...], norm_ref[0:1, 0:1]
    )
    for value, out in ((sol, sol_out), (res, res_out)):
        for j in range(TILES):
            width = min(LANES, NCOEF - j * LANES)
            out[:, j * LANES : j * LANES + width] = value[j * BANDS : (j + 1) * BANDS, :width]


VMEM = pl.BlockSpec(memory_space=pltpu.VMEM)
HBM = pl.BlockSpec(memory_space=pltpu.HBM)
LIMIT = 24 * 1024 * 1024


def shape(*dims, kind=F32):
    return jax.ShapeDtypeStruct(dims, kind)


def call(kernel, name, outs, ins, scratch=(), limit=LIMIT):
    return pl.pallas_call(
        kernel,
        name=name,
        out_shape=outs,
        in_specs=ins,
        out_specs=[VMEM] * len(outs),
        scratch_shapes=list(scratch),
        compiler_params=pltpu.CompilerParams(vmem_limit_bytes=limit),
    )


def sum_up(parts):
    total = parts[0]
    for i in range(1, parts.shape[0]):
        total = total + parts[i]
    return total


def device(y, z, x, c):
    return ((y * SPAN["z"] + z) * SPAN["x"] + x) * SPAN["c"] + c


def two_rounds():
    ys, zs, xs, pairs = range(SPAN["y"]), range(SPAN["z"]), range(SPAN["x"]), range(SPAN["y"] // 2)
    spread = sorted(zs, key=lambda z: (z % 4, z))
    halves = sorted(xs, key=lambda x: (x % 2, x))
    one = [[device(y, z, x, 0) for y in halves for x in halves] for z in zs]
    one += [[device(2 * pair + k, z, x, 1) for z in zs for k in (0, 1)] for x in xs for pair in pairs]
    two = [[device(y, z, x, 0) for z in spread] for y in ys for x in xs]
    two += [[device(y, z, x, 1) for x in xs for y in take] for z in zs for take in ((0, 3), (1, 2))]
    return one, two


def sent_to_all(block, groups):
    size = len(groups[0])
    sent = jnp.broadcast_to(block[None], (size, *block.shape))
    return sum_up(lax.all_to_all(sent, AXES, 0, 0, tiled=True, axis_index_groups=groups))


def summed(mine, other):
    swap = [(0, 1), (1, 0)]
    mine = mine + lax.ppermute(other, "c", swap)
    for groups in two_rounds():
        mine = sent_to_all(mine, groups)
    return mine, lax.ppermute(mine, "c", swap)


def body(basis, pixel_ids, band_ids, mags, inv_var):
    pixels = float(PIX * 256)
    objects = [a.reshape(OBJ_ROWS, LANES) for a in (pixel_ids, band_ids, mags, inv_var)]
    core = jnp.broadcast_to(lax.axis_index("c"), (8, LANES)).astype(jnp.int32)
    vec, half, norm_shape = shape(ROWS, LANES), shape(HALF, LANES), shape(8, LANES)
    scratch = [pltpu.VMEM((8, WIDE), F32), pltpu.VMEM((ROWS, LANES), F32)]
    copied, turned = shape(WIDE, PIX, kind=BF16), shape(PIX, WIDE, kind=BF16)
    mine, other, *fixed = call(
        first_kernel,
        "first",
        [half, half, shape(8, PIX), copied, copied, turned, turned],
        [VMEM] + [HBM] * 5,
        [
            pltpu.VMEM((NCOEF, PIX), F32),
            pltpu.VMEM((OBJ_ROWS, LANES), jnp.int32),
            pltpu.VMEM((OBJ_ROWS, LANES), jnp.int32),
            pltpu.VMEM((OBJ_ROWS, LANES), F32),
            pltpu.VMEM((OBJ_ROWS, LANES), F32),
            pltpu.VMEM((128, OBJ_ROWS * LANES), BF16),
            pltpu.VMEM((128, OBJ_ROWS * LANES), BF16),
            pltpu.VMEM((ROWS, LANES), F32),
            pltpu.SemaphoreType.DMA,
            pltpu.SemaphoreType.DMA((4,)),
        ],
    )(core, *[pltpu.with_memory_space_constraint(a, pltpu.HBM) for a in (basis.T, *objects)])
    mine, other, res, norm = call(
        functools.partial(start_kernel, pixels**0.5), "start", [half, half, vec, norm_shape], [VMEM] * 8, scratch
    )(core, *summed(mine, other), *fixed)
    sol, direction = jnp.zeros((ROWS, LANES), F32), res
    for _ in range(ITERS - 1):
        mine, other, sol, res, direction, norm = call(
            functools.partial(step_kernel, pixels), "step", [half, half, vec, vec, vec, norm_shape], [VMEM] * 12, scratch
        )(core, *summed(mine, other), sol, res, direction, norm, *fixed)
    out = shape(BANDS, NCOEF)
    return tuple(
        call(functools.partial(last_kernel, pixels), "last", [out, out], [VMEM] * 7)(
            core, *summed(mine, other), sol, res, direction, norm
        )
    )


def solution(mesh):
    torus = Mesh(mesh.devices.reshape(*(SPAN[a] for a in AXES)), AXES)
    return jax.shard_map(
        body,
        mesh=torus,
        in_specs=(P(AXES, None),) + (P(AXES),) * 4,
        out_specs=(P(), P()),
        check_vma=False,
    )
```
